512 devices in a mesh: obs: 16 (over z_hi, y, core), flux: 32 (over z_lo, x).
Axes of the slice: x: 4, y: 4, z: 16 (z_hi: 2, z_lo: 8; z = z_hi * 8 + z_lo), core: 2. Of those that a mesh axis runs over, the one named last changes fastest.
Arguments:
- jacobian: bfloat16 [2048, 32768], P('obs', 'flux'), may hold values from -0.03125 to 0.03125
- probes: bfloat16 [2, 32768, 128], P(None, 'flux'), may hold values from -6 to 6
- prior_std: float32 [32768], P('flux'), may hold values from 0.5 to 2
- obs_weight: float32 [2048], P('obs'), may hold values from 0.25 to 4
Outputs:
- sketch: float32 [32768, 256], P(('flux', 'obs'))
- basis_out: float32 [32768, 256], P(('flux', 'obs'))
The draws below stay inside these ranges and needn't reach their ends.
All inputs are finite; a program needn't handle non-finite values.
Results may differ from the reference program's by a relative error of at most 0.005.
Values may be sent and summed in bfloat16 or wider, within the bound.
No kernel may reach another device: no remote copies, remote signals or barrier semaphores. Data moves between devices by JAX's collectives and lax.ppermute only.
A program may use at most 64 MiB of HBM per device.

```python
import math
import jax
import jax.numpy as jnp
from jax import lax

P_SIZE = 128
NB = 2
OBS = 2048
FLUX = 32768


def level_of(own_key, extent, shards, least, high):
    loudness, own = 1.0, jax.random.fold_in(own_key, 6)
    for axis_at, parts in shards:
        steps = jnp.exp(jax.random.uniform(jax.random.fold_in(own, axis_at), (parts,), jnp.float32, least / len(shards), high / len(shards)))
        loudness = loudness * jnp.repeat(steps, extent[axis_at] // parts).reshape([-1 if axis == axis_at else 1 for axis in range(len(extent))])
    return loudness


def noise(own_key, dims, scale, limit, pieces=(), dtype=jnp.bfloat16):
    entries = scale * jax.random.normal(own_key, dims, jnp.float32)
    if pieces:
        entries = entries * level_of(own_key, dims, pieces, -0.22, 0.18)
    return jnp.clip(entries, -limit, limit).astype(dtype)


def setup_inputs(seed: int = 0) -> dict:
    splits = jax.random.split(jax.random.key(seed), 5)
    return {
        "jacobian": noise(splits[0], (OBS, FLUX), FLUX ** -0.5, 0.03125, ((0, 16), (1, 32))),
        "probes": noise(splits[1], (NB, FLUX, P_SIZE), 1.0, 6.0, ((1, 32),)),
        "prior_std": jnp.clip(jnp.exp(math.log(2.0) - 1.3862944 * jax.random.uniform(splits[2], (FLUX,), jnp.float32) ** level_of(splits[2], (FLUX,), ((0, 32),), -0.2, 0.2)), 0.5, 2.0),
        "obs_weight": jnp.clip(jnp.exp(math.log(4.0) - 2.7725887 * jax.random.uniform(splits[3], (OBS,), jnp.float32) ** level_of(splits[3], (OBS,), ((0, 16),), -0.2, 0.2)), 0.25, 4.0),
    }


def reference(jacobian, probes, prior_std, obs_weight):
    column_total = NB * P_SIZE
    stacked = jnp.transpose(probes.astype(jnp.float32), (1, 0, 2)).reshape(FLUX, column_total)
    stacked = (stacked * prior_std[:, None]).astype(jnp.bfloat16)
    forward = jnp.dot(jacobian.astype(jnp.float32), stacked.astype(jnp.float32), preferred_element_type=jnp.float32)
    weighted = (forward * obs_weight[:, None]).astype(jnp.bfloat16)
    adjoint = lax.dot_general(jacobian.astype(jnp.float32), weighted.astype(jnp.float32), (((0,), (0,)), ((), ())), preferred_element_type=jnp.float32)
    sketch = adjoint * prior_std[:, None]
    gram_matrix = jnp.dot(sketch.T.astype(jnp.float32), sketch.astype(jnp.float32), precision=lax.Precision.HIGHEST, preferred_element_type=jnp.float32)
    factor = jnp.linalg.cholesky(gram_matrix)
    basis_out = jax.scipy.linalg.solve_triangular(factor, sketch.T, lower=True).T * math.sqrt(FLUX)
    return (sketch, basis_out)
```

```python
import math

import jax
import jax.numpy as jnp
from jax import lax
from jax.sharding import Mesh, PartitionSpec as P

OBS_AXES = ("zh", "y", "c")
FLUX_AXES = ("zl", "x")
PLANE = ("y", "c", "x")
LINE = ("zh", "zl")


def scatter_sum(parts, axes):
    moved = lax.all_to_all(parts, axes, 0, 0, tiled=True)
    return jnp.sum(moved.astype(jnp.float32), axis=0)


def gather(piece, axes):
    count = lax.axis_size(axes)
    return lax.all_to_all(
        jnp.broadcast_to(piece[None], (count, *piece.shape)), axes, 0, 0, tiled=True
    )


def to_tiles(full):
    rows, cols = full.shape
    return full.reshape(rows // 8, 8, cols // 128, 128).transpose(0, 2, 1, 3).reshape(-1, 8, 128)


def from_tiles(tiles, rows, cols):
    return tiles.reshape(rows // 8, cols // 128, 8, 128).transpose(0, 2, 1, 3).reshape(rows, cols)


def body(jacobian, probes, prior_std, obs_weight):
    block_count, flux_local, probe_count = probes.shape
    obs_local = jacobian.shape[0]
    columns = block_count * probe_count
    obs_parts = lax.axis_size(OBS_AXES)
    scaled = (probes.astype(jnp.float32) * prior_std[None, :, None]).astype(jnp.bfloat16)
    stacked = jnp.transpose(scaled, (1, 0, 2)).reshape(flux_local, columns)
    partial = jnp.dot(jacobian, stacked, preferred_element_type=jnp.float32)
    tile = scatter_sum(to_tiles(partial), FLUX_AXES)
    row = lax.axis_index(FLUX_AXES) // (columns // 128) * 8
    weight = lax.dynamic_slice_in_dim(obs_weight, row, 8)
    weighted = from_tiles(
        gather((tile * weight[:, None]).astype(jnp.bfloat16), FLUX_AXES), obs_local, columns
    )
    adjoint = lax.dot_general(
        jacobian, weighted, (((0,), (0,)), ((), ())), preferred_element_type=jnp.float32
    ).astype(jnp.bfloat16)
    portion = flux_local // obs_parts
    adjoint = scatter_sum(adjoint.reshape(obs_parts, portion, columns), OBS_AXES)
    local_std = lax.dynamic_slice_in_dim(prior_std, lax.axis_index(OBS_AXES) * portion, portion)
    sketch = adjoint * local_std[:, None]
    gram = jnp.dot(
        sketch.T, sketch, precision=lax.Precision.HIGHEST, preferred_element_type=jnp.float32
    )
    slab = scatter_sum(gram.reshape(lax.axis_size(PLANE), -1, columns), PLANE)
    slab = jnp.sum(gather(slab, LINE), axis=0)
    gram = gather(slab, PLANE).reshape(columns, columns)
    factor = jnp.linalg.cholesky(gram)
    scale_root = math.sqrt(flux_local * lax.axis_size(FLUX_AXES))
    basis_out = jax.scipy.linalg.solve_triangular(factor, sketch.T, lower=True).T * scale_root
    return (sketch, basis_out)


def solution(mesh):
    split = Mesh(mesh.devices.reshape(2, 4, 2, 8, 4), ("zh", "y", "c", "zl", "x"))
    in_specs = (P(OBS_AXES, FLUX_AXES), P(None, FLUX_AXES, None), P(FLUX_AXES), P(OBS_AXES))
    out_specs = (P(FLUX_AXES + OBS_AXES, None), P(FLUX_AXES + OBS_AXES, None))
    return jax.shard_map(
        body, mesh=split, in_specs=in_specs, out_specs=out_specs, check_vma=False
    )
```

```python
import functools
import math

import jax
import jax.numpy as jnp
from jax import lax
from jax.experimental import pallas as pl
from jax.experimental.pallas import tpu as pltpu
from jax.sharding import Mesh, PartitionSpec as P

OBS_AXES = ("zh", "y", "c")
FLUX_AXES = ("zl", "x")
PLANE = ("y", "c", "x")
LINE = ("zh", "zl")
HALF = 128
STEP = 8
HIGHEST = lax.Precision.HIGHEST


def pick(values, index):
    return jnp.take_along_axis(values, index, axis=1, mode="promise_in_bounds")


def eliminate(diag, side, inverse, lanes):
    sub = lax.broadcasted_iota(jnp.int32, (STEP, HALF), 0)
    blocks = HALF // STEP
    for t in range(blocks):
        top = t * STEP
        head = diag[top : top + STEP, :]
        for k in range(STEP):
            lanes[k * STEP : (k + 1) * STEP, :] = pick(head, jnp.full((STEP, HALF), top + k, jnp.int32))
        entry = {}
        for k in range(STEP):
            for j in range(k, STEP):
                entry[j, k] = lanes[pl.ds(k * STEP + j, STEP, stride=0), :]
        rows = [[ref[pl.ds(top + k, STEP, stride=0), :] for ref in (diag, side, inverse)] for k in range(STEP)]
        for k in range(STEP):
            scale = lax.rsqrt(entry[k, k])
            rows[k] = [row * scale for row in rows[k]]
            mult = {j: entry[j, k] * scale for j in range(k + 1, STEP)}
            for j in range(k + 1, STEP):
                for i in range(j, STEP):
                    entry[i, j] = entry[i, j] - mult[i] * mult[j]
                rows[j] = [row - mult[j] * pivot for row, pivot in zip(rows[j], rows[k])]
            for ref, row in zip((side, inverse), rows[k][1:]):
                ref[top + k : top + k + 1, :] = row[:1, :]
        for block in range(t + 1, blocks):
            low = block * STEP
            index = sub + low
            work = [ref[low : low + STEP, :] for ref in (diag, side, inverse)]
            for k in range(STEP):
                mult = pick(rows[k][0], index)
                work = [row - mult * pivot for row, pivot in zip(work, rows[k])]
            for ref, row in zip((diag, side, inverse), work):
                ref[low : low + STEP, :] = row


def identity():
    shape = (HALF, HALF)
    return (lax.broadcasted_iota(jnp.int32, shape, 0) == lax.broadcasted_iota(jnp.int32, shape, 1)).astype(jnp.float32)


def dot(a, b, dims):
    return lax.dot_general(a, b, (dims, ((), ())), precision=HIGHEST, preferred_element_type=jnp.float32)


def basis_kernel(root, gram, sketch, out, diag, side, low, mixed, high, lanes):
    diag[...] = gram[:HALF, :HALF]
    side[...] = gram[:HALF, HALF:]
    low[...] = identity()
    eliminate(diag, side, low, lanes)
    upper = side[...]
    diag[...] = gram[HALF:, HALF:] - dot(upper, upper, ((0,), (0,)))
    mixed[...] = -dot(upper, low[...], ((0,), (0,)))
    high[...] = identity()
    eliminate(diag, mixed, high, lanes)
    first, second = sketch[:, :HALF], sketch[:, HALF:]
    out[:, :HALF] = root * dot(first, low[...], ((1,), (1,)))
    out[:, HALF:] = root * (dot(first, mixed[...], ((1,), (1,))) + dot(second, high[...], ((1,), (1,))))


def basis(gram, sketch, root):
    square = pltpu.VMEM((HALF, HALF), jnp.float32)
    vmem = pl.BlockSpec(memory_space=pltpu.VMEM)
    return pl.pallas_call(
        functools.partial(basis_kernel, root),
        out_shape=jax.ShapeDtypeStruct(sketch.shape, jnp.float32),
        in_specs=[vmem, vmem],
        out_specs=vmem,
        scratch_shapes=[square, square, square, square, square, pltpu.VMEM((STEP * STEP, HALF), jnp.float32)],
        name="cholesky_basis",
    )(gram, sketch)


def scatter_sum(parts, axes):
    moved = lax.all_to_all(parts, axes, 0, 0, tiled=True)
    return jnp.sum(moved.astype(jnp.float32), axis=0)


def gather(piece, axes):
    count = lax.axis_size(axes)
    return lax.all_to_all(
        jnp.broadcast_to(piece[None], (count, *piece.shape)), axes, 0, 0, tiled=True
    )


def to_tiles(full):
    rows, cols = full.shape
    return full.reshape(rows // 8, 8, cols // 128, 128).transpose(0, 2, 1, 3).reshape(-1, 8, 128)


def from_tiles(tiles, rows, cols):
    return tiles.reshape(rows // 8, cols // 128, 8, 128).transpose(0, 2, 1, 3).reshape(rows, cols)


def body(jacobian, probes, prior_std, obs_weight):
    block_count, flux_local, probe_count = probes.shape
    obs_local = jacobian.shape[0]
    columns = block_count * probe_count
    obs_parts = lax.axis_size(OBS_AXES)
    scaled = (probes.astype(jnp.float32) * prior_std[None, :, None]).astype(jnp.bfloat16)
    stacked = jnp.transpose(scaled, (1, 0, 2)).reshape(flux_local, columns)
    partial = jnp.dot(jacobian, stacked, preferred_element_type=jnp.float32)
    tile = scatter_sum(to_tiles(partial), FLUX_AXES)
    row = lax.axis_index(FLUX_AXES) // (columns // 128) * 8
    weight = lax.dynamic_slice_in_dim(obs_weight, row, 8)
    weighted = from_tiles(
        gather((tile * weight[:, None]).astype(jnp.bfloat16), FLUX_AXES), obs_local, columns
    )
    adjoint = lax.dot_general(
        jacobian, weighted, (((0,), (0,)), ((), ())), preferred_element_type=jnp.float32
    ).astype(jnp.bfloat16)
    portion = flux_local // obs_parts
    adjoint = scatter_sum(adjoint.reshape(obs_parts, portion, columns), OBS_AXES)
    local_std = lax.dynamic_slice_in_dim(prior_std, lax.axis_index(OBS_AXES) * portion, portion)
    sketch = adjoint * local_std[:, None]
    gram = jnp.dot(
        sketch.T, sketch, precision=lax.Precision.HIGHEST, preferred_element_type=jnp.float32
    )
    slab = scatter_sum(gram.reshape(lax.axis_size(PLANE), -1, columns), PLANE)
    slab = jnp.sum(gather(slab, LINE), axis=0)
    gram = gather(slab, PLANE).reshape(columns, columns)
    scale_root = math.sqrt(flux_local * lax.axis_size(FLUX_AXES))
    basis_out = basis(gram, sketch, scale_root)
    return (sketch, basis_out)


def solution(mesh):
    split = Mesh(mesh.devices.reshape(2, 4, 2, 8, 4), ("zh", "y", "c", "zl", "x"))
    in_specs = (P(OBS_AXES, FLUX_AXES), P(None, FLUX_AXES, None), P(FLUX_AXES), P(OBS_AXES))
    out_specs = (P(FLUX_AXES + OBS_AXES, None), P(FLUX_AXES + OBS_AXES, None))
    return jax.shard_map(
        body, mesh=split, in_specs=in_specs, out_specs=out_specs, check_vma=False
    )
```

```python
import functools
import math

import jax
import jax.numpy as jnp
from jax import lax
from jax.experimental import pallas as pl
from jax.experimental.pallas import tpu as pltpu
from jax.sharding import Mesh, PartitionSpec as P

OBS_AXES = ("zh", "y", "c")
FLUX_AXES = ("zl", "x")
NEAR_OBS = ("y", "c")
PLANE = ("y", "c", "x")
LINE = ("zh", "zl")
HALF = 128
STEP = 8
HIGHEST = lax.Precision.HIGHEST


def pick(values, index):
    return jnp.take_along_axis(values, index, axis=1, mode="promise_in_bounds")


def eliminate(diag, side, inverse, lanes):
    sub = lax.broadcasted_iota(jnp.int32, (STEP, HALF), 0)
    blocks = HALF // STEP
    for t in range(blocks):
        top = t * STEP
        head = diag[top : top + STEP, :]
        for k in range(STEP):
            lanes[k * STEP : (k + 1) * STEP, :] = pick(head, jnp.full((STEP, HALF), top + k, jnp.int32))
        entry = {}
        for k in range(STEP):
            for j in range(k, STEP):
                entry[j, k] = lanes[pl.ds(k * STEP + j, STEP, stride=0), :]
        rows = [[ref[pl.ds(top + k, STEP, stride=0), :] for ref in (diag, side, inverse)] for k in range(STEP)]
        for k in range(STEP):
            scale = lax.rsqrt(entry[k, k])
            rows[k] = [row * scale for row in rows[k]]
            mult = {j: entry[j, k] * scale for j in range(k + 1, STEP)}
            for j in range(k + 1, STEP):
                for i in range(j, STEP):
                    entry[i, j] = entry[i, j] - mult[i] * mult[j]
                rows[j] = [row - mult[j] * pivot for row, pivot in zip(rows[j], rows[k])]
            for ref, row in zip((side, inverse), rows[k][1:]):
                ref[top + k : top + k + 1, :] = row[:1, :]
        for block in range(t + 1, blocks):
            low = block * STEP
            index = sub + low
            work = [ref[low : low + STEP, :] for ref in (diag, side, inverse)]
            for k in range(STEP):
                mult = pick(rows[k][0], index)
                work = [row - mult * pivot for row, pivot in zip(work, rows[k])]
            for ref, row in zip((diag, side, inverse), work):
                ref[low : low + STEP, :] = row


def identity():
    shape = (HALF, HALF)
    return (lax.broadcasted_iota(jnp.int32, shape, 0) == lax.broadcasted_iota(jnp.int32, shape, 1)).astype(jnp.float32)


def dot(a, b, dims):
    return lax.dot_general(a, b, (dims, ((), ())), precision=HIGHEST, preferred_element_type=jnp.float32)


def basis_kernel(root, gram, sketch, out, diag, side, low, mixed, high, lanes):
    diag[...] = gram[:HALF, :HALF]
    side[...] = gram[:HALF, HALF:]
    low[...] = identity()
    eliminate(diag, side, low, lanes)
    upper = side[...]
    diag[...] = gram[HALF:, HALF:] - dot(upper, upper, ((0,), (0,)))
    mixed[...] = -dot(upper, low[...], ((0,), (0,)))
    high[...] = identity()
    eliminate(diag, mixed, high, lanes)
    first, second = sketch[:, :HALF], sketch[:, HALF:]
    out[:, :HALF] = root * dot(first, low[...], ((1,), (1,)))
    out[:, HALF:] = root * (dot(first, mixed[...], ((1,), (1,))) + dot(second, high[...], ((1,), (1,))))


def basis(gram, sketch, root):
    square = pltpu.VMEM((HALF, HALF), jnp.float32)
    vmem = pl.BlockSpec(memory_space=pltpu.VMEM)
    return pl.pallas_call(
        functools.partial(basis_kernel, root),
        out_shape=jax.ShapeDtypeStruct(sketch.shape, jnp.float32),
        in_specs=[vmem, vmem],
        out_specs=vmem,
        scratch_shapes=[square, square, square, square, square, pltpu.VMEM((STEP * STEP, HALF), jnp.float32)],
        name="cholesky_basis",
    )(gram, sketch)


def scatter_sum(parts, axes):
    moved = lax.all_to_all(parts, axes, 0, 0, tiled=True)
    return jnp.sum(moved.astype(jnp.float32), axis=0)


def gather(piece, axes):
    count = lax.axis_size(axes)
    return lax.all_to_all(
        jnp.broadcast_to(piece[None], (count, *piece.shape)), axes, 0, 0, tiled=True
    )


def to_tiles(full):
    rows, cols = full.shape
    return full.reshape(rows // 8, 8, cols // 128, 128).transpose(0, 2, 1, 3).reshape(-1, 8, 128)


def from_tiles(tiles, rows, cols):
    return tiles.reshape(rows // 8, cols // 128, 8, 128).transpose(0, 2, 1, 3).reshape(rows, cols)


def pull(jacobian, weighted):
    return lax.dot_general(
        jacobian, weighted, (((0,), (0,)), ((), ())), preferred_element_type=jnp.float32
    )


def body(jacobian, probes, prior_std, obs_weight):
    block_count, flux_local, probe_count = probes.shape
    obs_local = jacobian.shape[0]
    columns = block_count * probe_count
    obs_parts = lax.axis_size(OBS_AXES)
    half, far = flux_local // 2, lax.axis_index("zh")
    near_part = lax.dynamic_slice_in_dim(jacobian, far * half, half, 1)
    far_part = lax.ppermute(
        lax.dynamic_slice_in_dim(jacobian, (1 - far) * half, half, 1), "zh", ((0, 1), (1, 0))
    )
    scaled = (probes.astype(jnp.float32) * prior_std[None, :, None]).astype(jnp.bfloat16)
    stacked = jnp.transpose(scaled, (1, 0, 2)).reshape(flux_local, columns)
    partial = jnp.dot(jacobian, stacked, preferred_element_type=jnp.float32)
    tile = scatter_sum(to_tiles(partial), FLUX_AXES)
    row = lax.axis_index(FLUX_AXES) // (columns // 128) * 8
    weight = lax.dynamic_slice_in_dim(obs_weight, row, 8)
    weighted = gather((tile * weight[:, None]).astype(jnp.bfloat16), ("zh",) + FLUX_AXES)
    weighted = from_tiles(weighted, 2 * obs_local, columns)
    adjoint = pull(near_part, lax.dynamic_slice_in_dim(weighted, far * obs_local, obs_local))
    adjoint += pull(far_part, lax.dynamic_slice_in_dim(weighted, (1 - far) * obs_local, obs_local))
    portion = flux_local // obs_parts
    adjoint = scatter_sum(adjoint.astype(jnp.bfloat16).reshape(-1, portion, columns), NEAR_OBS)
    local_std = lax.dynamic_slice_in_dim(prior_std, lax.axis_index(OBS_AXES) * portion, portion)
    sketch = adjoint * local_std[:, None]
    gram = jnp.dot(
        sketch.T, sketch, precision=lax.Precision.HIGHEST, preferred_element_type=jnp.float32
    )
    slab = scatter_sum(gram.reshape(lax.axis_size(PLANE), -1, columns), PLANE)
    slab = jnp.sum(gather(slab, LINE), axis=0)
    gram = gather(slab, PLANE).reshape(columns, columns)
    scale_root = math.sqrt(flux_local * lax.axis_size(FLUX_AXES))
    return (sketch, basis(gram, sketch, scale_root))


def solution(mesh):
    split = Mesh(mesh.devices.reshape(2, 4, 2, 8, 4), ("zh", "y", "c", "zl", "x"))
    in_specs = (P(OBS_AXES, FLUX_AXES), P(None, FLUX_AXES, None), P(FLUX_AXES), P(OBS_AXES))
    out_specs = (P(FLUX_AXES + OBS_AXES, None), P(FLUX_AXES + OBS_AXES, None))
    return jax.shard_map(
        body, mesh=split, in_specs=in_specs, out_specs=out_specs, check_vma=False
    )
```

```python
import functools
import math

import jax
import jax.numpy as jnp
from jax import lax
from jax.experimental import pallas as pl
from jax.experimental.pallas import tpu as pltpu
from jax.sharding import Mesh, PartitionSpec as P

OBS_AXES = ("zh", "y", "c")
FLUX_AXES = ("zl", "x")
NEAR_OBS = ("y", "c")
PLANE = ("y", "c", "x")
LINE = ("zh", "zl")
HALF = 128
STEP = 8
HIGHEST = lax.Precision.HIGHEST


def pick(values, index):
    return jnp.take_along_axis(values, index, axis=1, mode="promise_in_bounds")


def eliminate(diag, side, inverse, lanes):
    sub = lax.broadcasted_iota(jnp.int32, (STEP, HALF), 0)
    blocks = HALF // STEP
    for t in range(blocks):
        top = t * STEP
        head = diag[top : top + STEP, :]
        for k in range(STEP):
            lanes[k * STEP : (k + 1) * STEP, :] = pick(head, jnp.full((STEP, HALF), top + k, jnp.int32))
        entry = {}
        for k in range(STEP):
            for j in range(k, STEP):
                entry[j, k] = lanes[pl.ds(k * STEP + j, STEP, stride=0), :]
        rows = [[ref[pl.ds(top + k, STEP, stride=0), :] for ref in (diag, side, inverse)] for k in range(STEP)]
        for k in range(STEP):
            scale = lax.rsqrt(entry[k, k])
            rows[k] = [row * scale for row in rows[k]]
            mult = {j: entry[j, k] * scale for j in range(k + 1, STEP)}
            for j in range(k + 1, STEP):
                for i in range(j, STEP):
                    entry[i, j] = entry[i, j] - mult[i] * mult[j]
                rows[j] = [row - mult[j] * pivot for row, pivot in zip(rows[j], rows[k])]
            for ref, row in zip((side, inverse), rows[k][1:]):
                ref[top + k : top + k + 1, :] = row[:1, :]
        for block in range(t + 1, blocks):
            low = block * STEP
            index = sub + low
            work = [ref[low : low + STEP, :] for ref in (diag, side, inverse)]
            for k in range(STEP):
                mult = pick(rows[k][0], index)
                work = [row - mult * pivot for row, pivot in zip(work, rows[k])]
            for ref, row in zip((diag, side, inverse), work):
                ref[low : low + STEP, :] = row


def identity():
    shape = (HALF, HALF)
    return (lax.broadcasted_iota(jnp.int32, shape, 0) == lax.broadcasted_iota(jnp.int32, shape, 1)).astype(jnp.float32)


def dot(a, b, dims):
    return lax.dot_general(a, b, (dims, ((), ())), precision=HIGHEST, preferred_element_type=jnp.float32)


def basis_kernel(root, gram, sketch, out, diag, side, low, mixed, high, lanes):
    diag[...] = gram[:HALF, :HALF]
    side[...] = gram[:HALF, HALF:]
    low[...] = identity()
    eliminate(diag, side, low, lanes)
    upper = side[...]
    diag[...] = gram[HALF:, HALF:] - dot(upper, upper, ((0,), (0,)))
    mixed[...] = -dot(upper, low[...], ((0,), (0,)))
    high[...] = identity()
    eliminate(diag, mixed, high, lanes)
    first, second = sketch[:, :HALF], sketch[:, HALF:]
    out[:, :HALF] = root * dot(first, low[...], ((1,), (1,)))
    out[:, HALF:] = root * (dot(first, mixed[...], ((1,), (1,))) + dot(second, high[...], ((1,), (1,))))


def basis(gram, sketch, root):
    square = pltpu.VMEM((HALF, HALF), jnp.float32)
    vmem = pl.BlockSpec(memory_space=pltpu.VMEM)
    return pl.pallas_call(
        functools.partial(basis_kernel, root),
        out_shape=jax.ShapeDtypeStruct(sketch.shape, jnp.float32),
        in_specs=[vmem, vmem],
        out_specs=vmem,
        scratch_shapes=[square, square, square, square, square, pltpu.VMEM((STEP * STEP, HALF), jnp.float32)],
        name="cholesky_basis",
    )(gram, sketch)


def scatter_sum(parts, axes):
    moved = lax.all_to_all(parts, axes, 0, 0, tiled=True)
    return jnp.sum(moved.astype(jnp.float32), axis=0)


def gather(piece, axes):
    count = lax.axis_size(axes)
    return lax.all_to_all(
        jnp.broadcast_to(piece[None], (count, *piece.shape)), axes, 0, 0, tiled=True
    )


def to_tiles(full):
    rows, cols = full.shape
    return full.reshape(rows // 8, 8, cols // 128, 128).transpose(0, 2, 1, 3).reshape(-1, 8, 128)


def from_tiles(tiles, rows, cols):
    return tiles.reshape(rows // 8, cols // 128, 8, 128).transpose(0, 2, 1, 3).reshape(rows, cols)


def pull(jacobian, weighted):
    return lax.dot_general(
        jacobian, weighted, (((0,), (0,)), ((), ())), preferred_element_type=jnp.float32
    )


def body(jacobian, probes, prior_std, obs_weight):
    block_count, flux_local, probe_count = probes.shape
    obs_local = jacobian.shape[0]
    columns = block_count * probe_count
    half, far = flux_local // 2, lax.axis_index("zh").astype(jnp.uint32)
    rows = (far * obs_local, (1 - far) * obs_local, far * half)
    portion = flux_local // lax.axis_size(OBS_AXES)
    local_std = lax.dynamic_slice_in_dim(prior_std, lax.axis_index(OBS_AXES) * portion, portion)
    row = lax.axis_index(FLUX_AXES) // (columns // 128) * 8
    weight = lax.dynamic_slice_in_dim(obs_weight, row, 8)
    sent = lax.dynamic_slice_in_dim(jacobian, (1 - far) * half, half, 1)
    scaled = (probes.astype(jnp.float32) * prior_std[None, :, None]).astype(jnp.bfloat16)
    stacked = jnp.transpose(scaled, (1, 0, 2)).reshape(flux_local, columns)
    stacked, weight, local_std, sent, rows = lax.optimization_barrier(
        (stacked, weight, local_std, sent, rows)
    )
    near_part = lax.dynamic_slice_in_dim(jacobian, rows[2], half, 1)
    far_part = lax.ppermute(sent, "zh", ((0, 1), (1, 0)))
    partial = jnp.dot(jacobian, stacked, preferred_element_type=jnp.float32)
    moved = lax.all_to_all(to_tiles(partial), FLUX_AXES, 0, 0, tiled=True)
    tile = jnp.sum(moved, axis=0)
    weighted = gather((tile * weight[:, None]).astype(jnp.bfloat16), ("zh",) + FLUX_AXES)
    weighted = from_tiles(weighted, 2 * obs_local, columns)
    adjoint = pull(near_part, lax.dynamic_slice_in_dim(weighted, rows[0], obs_local))
    adjoint += pull(far_part, lax.dynamic_slice_in_dim(weighted, rows[1], obs_local))
    adjoint = scatter_sum(adjoint.astype(jnp.bfloat16).reshape(-1, portion, columns), NEAR_OBS)
    sketch = adjoint * local_std[:, None]
    gram = jnp.dot(
        sketch.T, sketch, precision=lax.Precision.HIGHEST, preferred_element_type=jnp.float32
    )
    slab = scatter_sum(gram.reshape(lax.axis_size(PLANE), -1, columns), PLANE)
    slab = jnp.sum(gather(slab.astype(jnp.bfloat16), LINE).astype(jnp.float32), axis=0)
    gram = gather(slab, PLANE).reshape(columns, columns)
    scale_root = math.sqrt(flux_local * lax.axis_size(FLUX_AXES))
    return (sketch, basis(gram, sketch, scale_root))


def solution(mesh):
    split = Mesh(mesh.devices.reshape(2, 4, 2, 8, 4), ("zh", "y", "c", "zl", "x"))
    in_specs = (P(OBS_AXES, FLUX_AXES), P(None, FLUX_AXES, None), P(FLUX_AXES), P(OBS_AXES))
    out_specs = (P(FLUX_AXES + OBS_AXES, None), P(FLUX_AXES + OBS_AXES, None))

    return jax.shard_map(body, mesh=split, in_specs=in_specs, out_specs=out_specs, check_vma=False)
```

```python
import functools
import math

import jax
import jax.numpy as jnp
from jax import lax
from jax.experimental import pallas as pl
from jax.experimental.pallas import tpu as pltpu
from jax.sharding import Mesh, PartitionSpec as P

OBS_AXES = ("zh", "y", "c")
FLUX_AXES = ("zl", "x")
NEAR_OBS = ("y", "c")
PLANE = ("y", "c", "x")
LINE = ("zh", "zl")
HALF = 128
STEP = 8
HIGHEST = lax.Precision.HIGHEST


def pick(values, index):
    return jnp.take_along_axis(values, index, axis=1, mode="promise_in_bounds")


def eliminate(diag, side, inverse, lanes):
    sub = lax.broadcasted_iota(jnp.int32, (STEP, HALF), 0)
    blocks = HALF // STEP
    for t in range(blocks):
        top = t * STEP
        head = diag[top : top + STEP, :]
        for k in range(STEP):
            lanes[k * STEP : (k + 1) * STEP, :] = pick(head, jnp.full((STEP, HALF), top + k, jnp.int32))
        entry = {}
        for k in range(STEP):
            for j in range(k, STEP):
                entry[j, k] = lanes[pl.ds(k * STEP + j, STEP, stride=0), :]
        rows = [[ref[pl.ds(top + k, STEP, stride=0), :] for ref in (diag, side, inverse)] for k in range(STEP)]
        for k in range(STEP):
            scale = lax.rsqrt(entry[k, k])
            rows[k] = [row * scale for row in rows[k]]
            mult = {j: entry[j, k] * scale for j in range(k + 1, STEP)}
            for j in range(k + 1, STEP):
                for i in range(j, STEP):
                    entry[i, j] = entry[i, j] - mult[i] * mult[j]
                rows[j] = [row - mult[j] * pivot for row, pivot in zip(rows[j], rows[k])]
            for ref, row in zip((side, inverse), rows[k][1:]):
                ref[top + k : top + k + 1, :] = row[:1, :]
        for block in range(t + 1, blocks):
            low = block * STEP
            index = sub + low
            work = [ref[low : low + STEP, :] for ref in (diag, side, inverse)]
            for k in range(STEP):
                mult = pick(rows[k][0], index)
                work = [row - mult * pivot for row, pivot in zip(work, rows[k])]
            for ref, row in zip((diag, side, inverse), work):
                ref[low : low + STEP, :] = row


def identity():
    shape = (HALF, HALF)
    return (lax.broadcasted_iota(jnp.int32, shape, 0) == lax.broadcasted_iota(jnp.int32, shape, 1)).astype(jnp.float32)


def dot(a, b, dims):
    return lax.dot_general(a, b, (dims, ((), ())), precision=HIGHEST, preferred_element_type=jnp.float32)


def basis_kernel(root, gram, sketch, out, diag, side, low, mixed, high, lanes):
    diag[...] = gram[:HALF, :HALF]
    side[...] = gram[:HALF, HALF:]
    low[...] = identity()
    eliminate(diag, side, low, lanes)
    upper = side[...]
    diag[...] = gram[HALF:, HALF:] - dot(upper, upper, ((0,), (0,)))
    mixed[...] = -dot(upper, low[...], ((0,), (0,)))
    high[...] = identity()
    eliminate(diag, mixed, high, lanes)
    first, second = sketch[:, :HALF], sketch[:, HALF:]
    out[:, :HALF] = root * dot(first, low[...], ((1,), (1,)))
    out[:, HALF:] = root * (dot(first, mixed[...], ((1,), (1,))) + dot(second, high[...], ((1,), (1,))))


def basis(gram, sketch, root):
    square = pltpu.VMEM((HALF, HALF), jnp.float32)
    vmem = pl.BlockSpec(memory_space=pltpu.VMEM)
    return pl.pallas_call(
        functools.partial(basis_kernel, root),
        out_shape=jax.ShapeDtypeStruct(sketch.shape, jnp.float32),
        in_specs=[vmem, vmem],
        out_specs=vmem,
        scratch_shapes=[square, square, square, square, square, pltpu.VMEM((STEP * STEP, HALF), jnp.float32)],
        name="cholesky_basis",
    )(gram, sketch)


def forward_kernel(jacobian, probes, spread, out, stacked):
    sub = lax.broadcasted_iota(jnp.int32, (STEP, HALF), 0)
    blocks, flux_local, _ = probes.shape
    pair = 2 * STEP
    for low in range(0, flux_local, pair):
        row = spread[pl.ds(low // HALF, STEP, stride=0), :]
        factor = jnp.concatenate([pick(row, sub + (low + half) % HALF) for half in (0, STEP)], axis=0)
        for b in range(blocks):
            scaled = probes[b, low : low + pair, :].astype(jnp.float32) * factor
            stacked[low : low + pair, b * HALF : (b + 1) * HALF] = scaled.astype(jnp.bfloat16)
    total = jnp.dot(jacobian[...], stacked[...], preferred_element_type=jnp.float32)
    for k in range(out.shape[0]):
        r, c = k // blocks * STEP, k % blocks * HALF
        out[k] = total[r : r + STEP, c : c + HALF]


def forward_tiles(jacobian, probes, prior_std):
    rows, flux_local = jacobian.shape
    columns = probes.shape[0] * probes.shape[2]
    vmem = pl.BlockSpec(memory_space=pltpu.VMEM)
    return pl.pallas_call(
        forward_kernel,
        out_shape=jax.ShapeDtypeStruct((rows * columns // (STEP * HALF), STEP, HALF), jnp.float32),
        in_specs=[vmem, vmem, vmem],
        out_specs=vmem,
        scratch_shapes=[pltpu.VMEM((flux_local, columns), jnp.bfloat16)],
        name="forward_tiles",
    )(jacobian, probes, prior_std.reshape(flux_local // HALF, HALF))


def scatter_sum(parts, axes):
    moved = lax.all_to_all(parts, axes, 0, 0, tiled=True)
    return jnp.sum(moved.astype(jnp.float32), axis=0)


def gather(piece, axes):
    count = lax.axis_size(axes)
    return lax.all_to_all(
        jnp.broadcast_to(piece[None], (count, *piece.shape)), axes, 0, 0, tiled=True
    )


def from_tiles(tiles, rows, cols):
    return tiles.reshape(rows // 8, cols // 128, 8, 128).transpose(0, 2, 1, 3).reshape(rows, cols)


def pull(jacobian, weighted):
    return lax.dot_general(
        jacobian, weighted, (((0,), (0,)), ((), ())), preferred_element_type=jnp.float32
    )


def body(jacobian, probes, prior_std, obs_weight):
    flux_local = probes.shape[1]
    obs_local = jacobian.shape[0]
    columns = probes.shape[0] * probes.shape[2]
    half, far = flux_local // 2, lax.axis_index("zh").astype(jnp.uint32)
    rows = (far * obs_local, (1 - far) * obs_local, far * half)
    portion = flux_local // lax.axis_size(OBS_AXES)
    local_std = lax.dynamic_slice_in_dim(prior_std, lax.axis_index(OBS_AXES) * portion, portion)
    row = lax.axis_index(FLUX_AXES) // (columns // 128) * 8
    weight = lax.dynamic_slice_in_dim(obs_weight, row, 8)
    sent = lax.dynamic_slice_in_dim(jacobian, (1 - far) * half, half, 1)
    far_part = lax.ppermute(sent, "zh", ((0, 1), (1, 0)))
    tiles = forward_tiles(jacobian, probes, prior_std)
    moved = lax.all_to_all(tiles, FLUX_AXES, 0, 0, tiled=True)
    tile = jnp.sum(moved, axis=0)
    tile, weight, local_std, rows = lax.optimization_barrier((tile, weight, local_std, rows))
    near_part = lax.dynamic_slice_in_dim(jacobian, rows[2], half, 1)
    weighted = gather((tile * weight[:, None]).astype(jnp.bfloat16), ("zh",) + FLUX_AXES)
    weighted = from_tiles(weighted, 2 * obs_local, columns)
    adjoint = pull(near_part, lax.dynamic_slice_in_dim(weighted, rows[0], obs_local))
    adjoint += pull(far_part, lax.dynamic_slice_in_dim(weighted, rows[1], obs_local))
    adjoint = scatter_sum(adjoint.astype(jnp.bfloat16).reshape(-1, portion, columns), NEAR_OBS)
    sketch = adjoint * local_std[:, None]
    gram = jnp.dot(
        sketch.T, sketch, precision=lax.Precision.HIGHEST, preferred_element_type=jnp.float32
    )
    slab = scatter_sum(gram.astype(jnp.bfloat16).reshape(lax.axis_size(PLANE), -1, columns), PLANE)
    slab = lax.optimization_barrier(slab).astype(jnp.bfloat16)
    slab = jnp.sum(gather(slab, LINE).astype(jnp.float32), axis=0)
    gram = gather(slab, PLANE).reshape(columns, columns)
    scale_root = math.sqrt(flux_local * lax.axis_size(FLUX_AXES))
    return (sketch, basis(gram, sketch, scale_root))


def solution(mesh):
    split = Mesh(mesh.devices.reshape(2, 4, 2, 8, 4), ("zh", "y", "c", "zl", "x"))
    in_specs = (P(OBS_AXES, FLUX_AXES), P(None, FLUX_AXES, None), P(FLUX_AXES), P(OBS_AXES))
    out_specs = (P(FLUX_AXES + OBS_AXES, None), P(FLUX_AXES + OBS_AXES, None))

    return jax.shard_map(body, mesh=split, in_specs=in_specs, out_specs=out_specs, check_vma=False)
```

```python
import functools
import math

import jax
import jax.numpy as jnp
from jax import lax
from jax.experimental import pallas as pl
from jax.experimental.pallas import tpu as pltpu
from jax.sharding import Mesh, PartitionSpec as P

OBS_AXES = ("zh", "y", "c")
FLUX_AXES = ("zl", "x")
NEAR_OBS = ("y", "c")
PLANE = ("y", "c", "x")
LINE = ("zh", "zl")
HALF = 128
STEP = 8
VMEM_LIMIT = 16 * 2**20
HIGHEST = lax.Precision.HIGHEST


def pick(values, index):
    return jnp.take_along_axis(values, index, axis=1, mode="promise_in_bounds")


def eliminate(diag, side, inverse, lanes, near):
    sub = lax.broadcasted_iota(jnp.int32, (STEP, HALF), 0)
    blocks = HALF // STEP
    columns = [pick(diag[:STEP, :], jnp.full((STEP, HALF), k, jnp.int32)) for k in range(STEP)]
    for t in range(blocks):
        top, low = t * STEP, (t + 1) * STEP
        base = t % 2 * STEP * STEP
        for k in range(STEP):
            lanes[base + k * STEP : base + (k + 1) * STEP, :] = columns[k]
        entry = {}
        for k in range(STEP):
            for j in range(k, STEP):
                entry[j, k] = lanes[pl.ds(base + k * STEP + j, STEP, stride=0), :]
        rows = [[ref[pl.ds(top + k, STEP, stride=0), :] for ref in (diag, side, inverse)] for k in range(STEP)]
        last = t + 1 == blocks
        if not last:
            below = diag[low : low + STEP, :]
            columns = [pick(below, jnp.full((STEP, HALF), low + k, jnp.int32)) for k in range(STEP)]
        for k in range(STEP):
            scale = lax.rsqrt(entry[k, k])
            rows[k] = [row * scale for row in rows[k]]
            mult = {j: entry[j, k] * scale for j in range(k + 1, STEP)}
            for j in range(k + 1, STEP):
                for i in range(j, STEP):
                    entry[i, j] = entry[i, j] - mult[i] * mult[j]
                rows[j] = [row - mult[j] * pivot for row, pivot in zip(rows[j], rows[k])]
            for ref, row in zip((side, inverse), rows[k][1:]):
                ref[top + k : top + k + 1, :] = row[:1, :]
            if not last:
                mult = pick(rows[k][0], sub + low)
                spot = base + k * STEP
                near[spot : spot + STEP, :] = mult
                columns = [
                    column - mult * near[pl.ds(spot + j, STEP, stride=0), :]
                    for j, column in enumerate(columns)
                ]
        for block in range(t + 1, blocks):
            low = block * STEP
            index = sub + low
            work = [ref[low : low + STEP, :] for ref in (diag, side, inverse)]
            for k in range(STEP):
                if block == t + 1:
                    mult = near[base + k * STEP : base + (k + 1) * STEP, :]
                else:
                    mult = pick(rows[k][0], index)
                work = [row - mult * pivot for row, pivot in zip(work, rows[k])]
            for ref, row in zip((diag, side, inverse), work):
                ref[low : low + STEP, :] = row


def identity():
    shape = (HALF, HALF)
    return (lax.broadcasted_iota(jnp.int32, shape, 0) == lax.broadcasted_iota(jnp.int32, shape, 1)).astype(jnp.float32)


def dot(a, b, dims):
    return lax.dot_general(a, b, (dims, ((), ())), precision=HIGHEST, preferred_element_type=jnp.float32)


def basis_kernel(root, gram, sketch, out, diag, side, low, mixed, high, lanes, near):
    diag[...] = gram[:HALF, :HALF]
    side[...] = gram[:HALF, HALF:]
    low[...] = identity()
    eliminate(diag, side, low, lanes, near)
    upper = side[...]
    diag[...] = gram[HALF:, HALF:] - dot(upper, upper, ((0,), (0,)))
    mixed[...] = -dot(upper, low[...], ((0,), (0,)))
    high[...] = identity()
    eliminate(diag, mixed, high, lanes, near)
    first, second = sketch[:, :HALF], sketch[:, HALF:]
    out[:, :HALF] = root * dot(first, low[...], ((1,), (1,)))
    out[:, HALF:] = root * (dot(first, mixed[...], ((1,), (1,))) + dot(second, high[...], ((1,), (1,))))


def basis(gram, sketch, root):
    square = pltpu.VMEM((HALF, HALF), jnp.float32)
    vmem = pl.BlockSpec(memory_space=pltpu.VMEM)
    return pl.pallas_call(
        functools.partial(basis_kernel, root),
        out_shape=jax.ShapeDtypeStruct(sketch.shape, jnp.float32),
        in_specs=[vmem, vmem],
        out_specs=vmem,
        scratch_shapes=[square, square, square, square, square, *[pltpu.VMEM((2 * STEP * STEP, HALF), jnp.float32)] * 2],
        compiler_params=pltpu.CompilerParams(vmem_limit_bytes=VMEM_LIMIT),
        name="cholesky_basis",
    )(gram, sketch)


def forward_kernel(jacobian, probes, spread, out, stacked):
    sub = lax.broadcasted_iota(jnp.int32, (STEP, HALF), 0)
    blocks, flux_local, _ = probes.shape
    pair = 2 * STEP
    for low in range(0, flux_local, pair):
        row = spread[pl.ds(low // HALF, STEP, stride=0), :]
        factor = jnp.concatenate([pick(row, sub + (low + half) % HALF) for half in (0, STEP)], axis=0)
        for b in range(blocks):
            scaled = probes[b, low : low + pair, :].astype(jnp.float32) * factor
            stacked[low : low + pair, b * HALF : (b + 1) * HALF] = scaled.astype(jnp.bfloat16)
    total = jnp.dot(jacobian[...], stacked[...], preferred_element_type=jnp.float32)
    for k in range(out.shape[0]):
        r, c = k // blocks * STEP, k % blocks * HALF
        out[k] = total[r : r + STEP, c : c + HALF]


def forward_tiles(jacobian, probes, prior_std):
    rows, flux_local = jacobian.shape
    columns = probes.shape[0] * probes.shape[2]
    vmem = pl.BlockSpec(memory_space=pltpu.VMEM)
    return pl.pallas_call(
        forward_kernel,
        out_shape=jax.ShapeDtypeStruct((rows * columns // (STEP * HALF), STEP, HALF), jnp.float32),
        in_specs=[vmem, vmem, vmem],
        out_specs=vmem,
        scratch_shapes=[pltpu.VMEM((flux_local, columns), jnp.bfloat16)],
        name="forward_tiles",
    )(jacobian, probes, prior_std.reshape(flux_local // HALF, HALF))


def scatter_sum(parts, axes):
    moved = lax.all_to_all(parts, axes, 0, 0, tiled=True)
    return jnp.sum(moved.astype(jnp.float32), axis=0)


def gather(piece, axes):
    count = lax.axis_size(axes)
    return lax.all_to_all(
        jnp.broadcast_to(piece[None], (count, *piece.shape)), axes, 0, 0, tiled=True
    )


def from_tiles(tiles, rows, cols):
    return tiles.reshape(rows // 8, cols // 128, 8, 128).transpose(0, 2, 1, 3).reshape(rows, cols)


def pull(jacobian, weighted):
    return lax.dot_general(
        jacobian, weighted, (((0,), (0,)), ((), ())), preferred_element_type=jnp.float32
    )


def body(jacobian, probes, prior_std, obs_weight):
    flux_local = probes.shape[1]
    obs_local = jacobian.shape[0]
    columns = probes.shape[0] * probes.shape[2]
    half, far = flux_local // 2, lax.axis_index("zh").astype(jnp.uint32)
    rows = (far * obs_local, (1 - far) * obs_local, far * half)
    portion = flux_local // lax.axis_size(OBS_AXES)
    local_std = lax.dynamic_slice_in_dim(prior_std, lax.axis_index(OBS_AXES) * portion, portion)
    row = lax.axis_index(FLUX_AXES) // (columns // 128) * 8
    weight = lax.dynamic_slice_in_dim(obs_weight, row, 8)
    sent = lax.dynamic_slice_in_dim(jacobian, (1 - far) * half, half, 1)
    far_part = lax.ppermute(sent, "zh", ((0, 1), (1, 0)))
    tiles = forward_tiles(jacobian, probes, prior_std)
    moved = lax.all_to_all(tiles, FLUX_AXES, 0, 0, tiled=True)
    tile = jnp.sum(moved, axis=0)
    tile, weight, local_std, rows = lax.optimization_barrier((tile, weight, local_std, rows))
    near_part = lax.dynamic_slice_in_dim(jacobian, rows[2], half, 1)
    weighted = gather((tile * weight[:, None]).astype(jnp.bfloat16), ("zh",) + FLUX_AXES)
    weighted = from_tiles(weighted, 2 * obs_local, columns)
    adjoint = pull(near_part, lax.dynamic_slice_in_dim(weighted, rows[0], obs_local))
    adjoint += pull(far_part, lax.dynamic_slice_in_dim(weighted, rows[1], obs_local))
    adjoint = scatter_sum(adjoint.astype(jnp.bfloat16).reshape(-1, portion, columns), NEAR_OBS)
    sketch = adjoint * local_std[:, None]
    gram = jnp.dot(
        sketch.T, sketch, precision=lax.Precision.HIGHEST, preferred_element_type=jnp.float32
    )
    slab = scatter_sum(gram.astype(jnp.bfloat16).reshape(lax.axis_size(PLANE), -1, columns), PLANE)
    slab = lax.optimization_barrier(slab).astype(jnp.bfloat16)
    slab = jnp.sum(gather(slab, LINE).astype(jnp.float32), axis=0)
    gram = gather(slab, PLANE).reshape(columns, columns)
    scale_root = math.sqrt(flux_local * lax.axis_size(FLUX_AXES))
    return (sketch, basis(gram, sketch, scale_root))


def solution(mesh):
    split = Mesh(mesh.devices.reshape(2, 4, 2, 8, 4), ("zh", "y", "c", "zl", "x"))
    in_specs = (P(OBS_AXES, FLUX_AXES), P(None, FLUX_AXES, None), P(FLUX_AXES), P(OBS_AXES))
    out_specs = (P(FLUX_AXES + OBS_AXES, None), P(FLUX_AXES + OBS_AXES, None))

    return jax.shard_map(body, mesh=split, in_specs=in_specs, out_specs=out_specs, check_vma=False)
```

```python
import functools
import math

import jax
import jax.numpy as jnp
from jax import lax
from jax.experimental import pallas as pl
from jax.experimental.pallas import tpu as pltpu
from jax.sharding import Mesh, PartitionSpec as P

OBS_AXES = ("zh", "y", "c")
FLUX_AXES = ("zl", "x")
NEAR_OBS = ("y", "c")
PLANE = ("y", "c", "x")
LINE = ("zh", "zl")
HALF = 128
STEP = 8
CHUNKS = 4
VMEM_LIMIT = 16 * 2**20
HIGHEST = lax.Precision.HIGHEST


def pick(values, index):
    return jnp.take_along_axis(values, index, axis=1, mode="promise_in_bounds")


def eliminate(diag, inverse, lanes, near):
    sub = lax.broadcasted_iota(jnp.int32, (STEP, HALF), 0)
    blocks = HALF // STEP
    columns = [pick(diag[:STEP, :], jnp.full((STEP, HALF), k, jnp.int32)) for k in range(STEP)]
    for t in range(blocks):
        top, low = t * STEP, (t + 1) * STEP
        base = t % 2 * STEP * STEP
        for k in range(STEP):
            lanes[base + k * STEP : base + (k + 1) * STEP, :] = columns[k]
        entry = {}
        for k in range(STEP):
            for j in range(k, STEP):
                entry[j, k] = lanes[pl.ds(base + k * STEP + j, STEP, stride=0), :]
        rows = [[ref[pl.ds(top + k, STEP, stride=0), :] for ref in (diag, inverse)] for k in range(STEP)]
        last = t + 1 == blocks
        if not last:
            below = diag[low : low + STEP, :]
            columns = [pick(below, jnp.full((STEP, HALF), low + k, jnp.int32)) for k in range(STEP)]
        for k in range(STEP):
            scale = lax.rsqrt(entry[k, k])
            rows[k] = [row * scale for row in rows[k]]
            mult = {j: entry[j, k] * scale for j in range(k + 1, STEP)}
            for j in range(k + 1, STEP):
                for i in range(j, STEP):
                    entry[i, j] = entry[i, j] - mult[i] * mult[j]
                rows[j] = [row - mult[j] * pivot for row, pivot in zip(rows[j], rows[k])]
            for ref, row in zip((inverse,), rows[k][1:]):
                ref[top + k : top + k + 1, :] = row[:1, :]
            if not last:
                mult = pick(rows[k][0], sub + low)
                spot = base + k * STEP
                near[spot : spot + STEP, :] = mult
                columns = [
                    column - mult * near[pl.ds(spot + j, STEP, stride=0), :]
                    for j, column in enumerate(columns)
                ]
        for block in range(t + 1, blocks):
            low = block * STEP
            index = sub + low
            work = [ref[low : low + STEP, :] for ref in (diag, inverse)]
            for k in range(STEP):
                if block == t + 1:
                    mult = near[base + k * STEP : base + (k + 1) * STEP, :]
                else:
                    mult = pick(rows[k][0], index)
                work = [row - mult * pivot for row, pivot in zip(work, rows[k])]
            for ref, row in zip((diag, inverse), work):
                ref[low : low + STEP, :] = row


def identity():
    shape = (HALF, HALF)
    return (lax.broadcasted_iota(jnp.int32, shape, 0) == lax.broadcasted_iota(jnp.int32, shape, 1)).astype(jnp.float32)


def dot(a, b, dims):
    return lax.dot_general(a, b, (dims, ((), ())), precision=HIGHEST, preferred_element_type=jnp.float32)


def basis_kernel(root, gram, sketch, out, diag, low, high, lanes, near):
    diag[...] = gram[:HALF, :HALF]
    low[...] = identity()
    eliminate(diag, low, lanes, near)
    upper = dot(low[...], gram[:HALF, HALF:], ((1,), (0,)))
    diag[...] = gram[HALF:, HALF:] - dot(upper, upper, ((0,), (0,)))
    high[...] = identity()
    eliminate(diag, high, lanes, near)
    first, second = sketch[:, :HALF], sketch[:, HALF:]
    left = dot(first, low[...], ((1,), (1,)))
    out[:, :HALF] = root * left
    rest = second - dot(left, upper, ((1,), (0,)))
    out[:, HALF:] = root * dot(rest, high[...], ((1,), (1,)))


def basis(gram, sketch, root):
    square = pltpu.VMEM((HALF, HALF), jnp.float32)
    vmem = pl.BlockSpec(memory_space=pltpu.VMEM)
    return pl.pallas_call(
        functools.partial(basis_kernel, root),
        out_shape=jax.ShapeDtypeStruct(sketch.shape, jnp.float32),
        in_specs=[vmem, vmem],
        out_specs=vmem,
        scratch_shapes=[square, square, square, *[pltpu.VMEM((2 * STEP * STEP, HALF), jnp.float32)] * 2],
        compiler_params=pltpu.CompilerParams(vmem_limit_bytes=VMEM_LIMIT),
        name="cholesky_basis",
    )(gram, sketch)


def forward_kernel(
    far_jacobian, far_probes, far_spread, far_weight, far_out, jacobian, probes, spread, weight, stacked, out, sems
):
    sub = lax.broadcasted_iota(jnp.int32, (STEP, HALF), 0)
    blocks, flux_local, _ = probes.shape
    pair, chunk = 2 * STEP, flux_local // CHUNKS
    copies = [pltpu.make_async_copy(far_spread, spread, sems.at[CHUNKS])]
    for c in range(CHUNKS):
        part = (slice(None), pl.ds(c * chunk, chunk), slice(None))
        copies.append(pltpu.make_async_copy(far_probes.at[part], probes.at[part], sems.at[c]))
    copies.append(pltpu.make_async_copy(far_weight, weight, sems.at[CHUNKS + 2]))
    copies.append(pltpu.make_async_copy(far_jacobian, jacobian, sems.at[CHUNKS + 1]))
    for copy in copies:
        copy.start()
    copies[0].wait()
    for low in range(0, flux_local, pair):
        if low % chunk == 0:
            copies[1 + low // chunk].wait()
        row = spread[pl.ds(low // HALF, STEP, stride=0), :]
        factor = jnp.concatenate([pick(row, sub + (low + half) % HALF) for half in (0, STEP)], axis=0)
        for b in range(blocks):
            scaled = probes[b, low : low + pair, :].astype(jnp.float32) * factor
            stacked[low : low + pair, b * HALF : (b + 1) * HALF] = scaled.astype(jnp.bfloat16)
    copies[-2].wait()
    row = weight[pl.ds(0, STEP, stride=0), :]
    copies[-1].wait()
    total = jnp.dot(jacobian[...], stacked[...], preferred_element_type=jnp.float32)
    for k in range(out.shape[0]):
        r, c = k // blocks * STEP, k % blocks * HALF
        out[k] = total[r : r + STEP, c : c + HALF] * pick(row, sub + r)
    result = pltpu.make_async_copy(out, far_out, sems.at[CHUNKS])
    result.start()
    result.wait()


def forward_tiles(jacobian, probes, prior_std, obs_weight):
    rows, flux_local = jacobian.shape
    columns = probes.shape[0] * probes.shape[2]
    spread = prior_std.reshape(flux_local // HALF, HALF)
    hbm = pl.BlockSpec(memory_space=pltpu.MemorySpace.HBM)
    shape = (rows * columns // (STEP * HALF), STEP, HALF)
    return pl.pallas_call(
        forward_kernel,
        out_shape=jax.ShapeDtypeStruct(shape, jnp.float32),
        in_specs=[hbm] * 4,
        out_specs=hbm,
        scratch_shapes=[
            pltpu.VMEM(jacobian.shape, jacobian.dtype),
            pltpu.VMEM(probes.shape, probes.dtype),
            pltpu.VMEM(spread.shape, spread.dtype),
            pltpu.VMEM((1, rows), jnp.float32),
            pltpu.VMEM((flux_local, columns), jnp.bfloat16),
            pltpu.VMEM(shape, jnp.float32),
            pltpu.SemaphoreType.DMA((CHUNKS + 3,)),
        ],
        name="forward_tiles",
    )(jacobian, probes, spread, obs_weight.reshape(1, rows))


def scatter_sum(parts, axes):
    moved = lax.all_to_all(parts, axes, 0, 0, tiled=True)
    return jnp.sum(moved.astype(jnp.float32), axis=0)


def gather(piece, axes):
    count = lax.axis_size(axes)
    return lax.all_to_all(
        jnp.broadcast_to(piece[None], (count, *piece.shape)), axes, 0, 0, tiled=True
    )


def from_tiles(tiles, rows, cols):
    return tiles.reshape(rows // 8, cols // 128, 8, 128).transpose(0, 2, 1, 3).reshape(rows, cols)


def pull(jacobian, weighted):
    return lax.dot_general(
        jacobian, weighted, (((0,), (0,)), ((), ())), preferred_element_type=jnp.float32
    )


def body(jacobian, probes, prior_std, obs_weight):
    flux_local = probes.shape[1]
    obs_local = jacobian.shape[0]
    columns = probes.shape[0] * probes.shape[2]
    half, far = flux_local // 2, lax.axis_index("zh").astype(jnp.uint32)
    rows = (far * obs_local, (1 - far) * obs_local, far * half)
    portion = flux_local // lax.axis_size(OBS_AXES)
    local_std = lax.dynamic_slice_in_dim(prior_std, lax.axis_index(OBS_AXES) * portion, portion)
    sent = lax.dynamic_slice_in_dim(jacobian, (1 - far) * half, half, 1)
    far_part = lax.ppermute(sent, "zh", ((0, 1), (1, 0)))
    tiles = forward_tiles(jacobian, probes, prior_std, obs_weight)
    moved = lax.all_to_all(tiles, FLUX_AXES, 0, 0, tiled=True)
    tile = jnp.sum(moved, axis=0)
    tile, local_std, rows = lax.optimization_barrier((tile, local_std, rows))
    near_part = lax.dynamic_slice_in_dim(jacobian, rows[2], half, 1)
    weighted = gather(tile.astype(jnp.bfloat16), ("zh",) + FLUX_AXES)
    weighted = from_tiles(weighted, 2 * obs_local, columns)
    adjoint = pull(near_part, lax.dynamic_slice_in_dim(weighted, rows[0], obs_local))
    adjoint += pull(far_part, lax.dynamic_slice_in_dim(weighted, rows[1], obs_local))
    adjoint = scatter_sum(adjoint.astype(jnp.bfloat16).reshape(-1, portion, columns), NEAR_OBS)
    sketch = adjoint * local_std[:, None]
    gram = jnp.dot(
        sketch.T, sketch, precision=lax.Precision.HIGHEST, preferred_element_type=jnp.float32
    )
    slab = scatter_sum(gram.astype(jnp.bfloat16).reshape(lax.axis_size(PLANE), -1, columns), PLANE)
    slab = lax.optimization_barrier(slab).astype(jnp.bfloat16)
    slab = jnp.sum(gather(slab, LINE).astype(jnp.float32), axis=0)
    gram = gather(slab, PLANE).reshape(columns, columns)
    scale_root = math.sqrt(flux_local * lax.axis_size(FLUX_AXES))
    return (sketch, basis(gram, sketch, scale_root))


def solution(mesh):
    split = Mesh(mesh.devices.reshape(2, 4, 2, 8, 4), ("zh", "y", "c", "zl", "x"))
    in_specs = (P(OBS_AXES, FLUX_AXES), P(None, FLUX_AXES, None), P(FLUX_AXES), P(OBS_AXES))
    out_specs = (P(FLUX_AXES + OBS_AXES, None), P(FLUX_AXES + OBS_AXES, None))

    return jax.shard_map(body, mesh=split, in_specs=in_specs, out_specs=out_specs, check_vma=False)
```

```python
import functools
import math

import jax
import jax.numpy as jnp
from jax import lax
from jax.experimental import pallas as pl
from jax.experimental.pallas import tpu as pltpu
from jax.sharding import Mesh, PartitionSpec as P

OBS_AXES = ("zh", "y", "c")
FLUX_AXES = ("zl", "x")
NEAR_OBS = ("y", "c")
PLANE = ("y", "c", "x")
LINE = ("zh", "zl")
HALF = 128
STEP = 8
VMEM_LIMIT = 16 * 2**20
HIGHEST = lax.Precision.HIGHEST


def pick(values, index):
    return jnp.take_along_axis(values, index, axis=1, mode="promise_in_bounds")


def eliminate(diag, inverse, lanes, near):
    sub = lax.broadcasted_iota(jnp.int32, (STEP, HALF), 0)
    blocks = HALF // STEP
    columns = [pick(diag[:STEP, :], jnp.full((STEP, HALF), k, jnp.int32)) for k in range(STEP)]
    for t in range(blocks):
        top, low = t * STEP, (t + 1) * STEP
        base = t % 2 * STEP * STEP
        for k in range(STEP):
            lanes[base + k * STEP : base + (k + 1) * STEP, :] = columns[k]
        entry = {}
        for k in range(STEP):
            for j in range(k, STEP):
                entry[j, k] = lanes[pl.ds(base + k * STEP + j, STEP, stride=0), :]
        rows = [[ref[pl.ds(top + k, STEP, stride=0), :] for ref in (diag, inverse)] for k in range(STEP)]
        last = t + 1 == blocks
        if not last:
            below = diag[low : low + STEP, :]
            columns = [pick(below, jnp.full((STEP, HALF), low + k, jnp.int32)) for k in range(STEP)]
        for k in range(STEP):
            scale = lax.rsqrt(entry[k, k])
            rows[k] = [row * scale for row in rows[k]]
            mult = {j: entry[j, k] * scale for j in range(k + 1, STEP)}
            for j in range(k + 1, STEP):
                for i in range(j, STEP):
                    entry[i, j] = entry[i, j] - mult[i] * mult[j]
                rows[j] = [row - mult[j] * pivot for row, pivot in zip(rows[j], rows[k])]
            for ref, row in zip((inverse,), rows[k][1:]):
                ref[top + k : top + k + 1, :] = row[:1, :]
            if not last:
                mult = pick(rows[k][0], sub + low)
                spot = base + k * STEP
                near[spot : spot + STEP, :] = mult
                columns = [
                    column - mult * near[pl.ds(spot + j, STEP, stride=0), :]
                    for j, column in enumerate(columns)
                ]
        for block in range(t + 1, blocks):
            low = block * STEP
            index = sub + low
            work = [ref[low : low + STEP, :] for ref in (diag, inverse)]
            for k in range(STEP):
                if block == t + 1:
                    mult = near[base + k * STEP : base + (k + 1) * STEP, :]
                else:
                    mult = pick(rows[k][0], index)
                work = [row - mult * pivot for row, pivot in zip(work, rows[k])]
            for ref, row in zip((diag, inverse), work):
                ref[low : low + STEP, :] = row


def identity():
    shape = (HALF, HALF)
    return (lax.broadcasted_iota(jnp.int32, shape, 0) == lax.broadcasted_iota(jnp.int32, shape, 1)).astype(jnp.float32)


def dot(a, b, dims):
    return lax.dot_general(a, b, (dims, ((), ())), precision=HIGHEST, preferred_element_type=jnp.float32)


def basis_kernel(root, packed, sketch, out, gram, diag, low, high, lanes, near):
    rows = packed.shape[1]
    for k in range(packed.shape[0]):
        gram[k * rows : (k + 1) * rows, :] = packed[k]
    diag[...] = gram[:, :HALF]
    low[...] = identity()
    eliminate(diag, low, lanes, near)
    upper = dot(low[...], gram[:, HALF : 2 * HALF], ((1,), (0,)))
    diag[...] = gram[:, 2 * HALF :] - dot(upper, upper, ((0,), (0,)))
    high[...] = identity()
    eliminate(diag, high, lanes, near)
    first, second = sketch[:, :HALF], sketch[:, HALF:]
    left = dot(first, low[...], ((1,), (1,)))
    out[:, :HALF] = root * left
    rest = second - dot(left, upper, ((1,), (0,)))
    out[:, HALF:] = root * dot(rest, high[...], ((1,), (1,)))


def basis(gram, sketch, root):
    square = pltpu.VMEM((HALF, HALF), jnp.float32)
    vmem = pl.BlockSpec(memory_space=pltpu.VMEM)
    return pl.pallas_call(
        functools.partial(basis_kernel, root),
        out_shape=jax.ShapeDtypeStruct(sketch.shape, jnp.float32),
        in_specs=[vmem, vmem],
        out_specs=vmem,
        scratch_shapes=[pltpu.VMEM((HALF, 3 * HALF), jnp.float32), square, square, square, *[pltpu.VMEM((2 * STEP * STEP, HALF), jnp.float32)] * 2],
        compiler_params=pltpu.CompilerParams(vmem_limit_bytes=VMEM_LIMIT),
        name="cholesky_basis",
    )(gram, sketch)


def forward_kernel(
    far_jacobian, far_probes, far_spread, far_weight, far_out, jacobian, probes, spread, weight, out, sems
):
    sub = lax.broadcasted_iota(jnp.int32, (STEP, HALF), 0)
    blocks, flux_local, _ = probes.shape
    pair = 2 * STEP
    pairs = ((far_spread, spread), (far_probes, probes), (far_jacobian, jacobian), (far_weight, weight))
    copies = [pltpu.make_async_copy(*ends, sems.at[i]) for i, ends in enumerate(pairs)]
    for copy in copies:
        copy.start()
    for copy in copies:
        copy.wait()
    stacked = []
    for low in range(0, flux_local, pair):
        row = spread[pl.ds(low // HALF, STEP, stride=0), :]
        factor = jnp.concatenate([pick(row, sub + (low + half) % HALF) for half in (0, STEP)], axis=0)
        scaled = [probes[b, low : low + pair, :].astype(jnp.float32) * factor for b in range(blocks)]
        stacked.append(jnp.concatenate([block.astype(jnp.bfloat16) for block in scaled], axis=1))
    stacked = jnp.concatenate(stacked, axis=0)
    row = weight[pl.ds(0, STEP, stride=0), :]
    total = jnp.dot(jacobian[...], stacked, preferred_element_type=jnp.float32)
    for k in range(out.shape[0]):
        r, c = k // blocks * STEP, k % blocks * HALF
        out[k] = total[r : r + STEP, c : c + HALF] * pick(row, sub + r)
    result = pltpu.make_async_copy(out, far_out, sems.at[0])
    result.start()
    result.wait()


def forward_tiles(jacobian, probes, prior_std, obs_weight):
    rows, flux_local = jacobian.shape
    columns = probes.shape[0] * probes.shape[2]
    spread = prior_std.reshape(flux_local // HALF, HALF)
    hbm = pl.BlockSpec(memory_space=pltpu.MemorySpace.HBM)
    shape = (rows * columns // (STEP * HALF), STEP, HALF)
    return pl.pallas_call(
        forward_kernel,
        out_shape=jax.ShapeDtypeStruct(shape, jnp.float32),
        in_specs=[hbm] * 4,
        out_specs=hbm,
        scratch_shapes=[
            pltpu.VMEM(jacobian.shape, jacobian.dtype),
            pltpu.VMEM(probes.shape, probes.dtype),
            pltpu.VMEM(spread.shape, spread.dtype),
            pltpu.VMEM((1, rows), jnp.float32),
            pltpu.VMEM(shape, jnp.float32),
            pltpu.SemaphoreType.DMA((4,)),
        ],
        name="forward_tiles",
    )(jacobian, probes, spread, obs_weight.reshape(1, rows))


def scatter_sum(parts, axes):
    moved = lax.all_to_all(parts, axes, 0, 0, tiled=True)
    return jnp.sum(moved.astype(jnp.float32), axis=0)


def gather(piece, axes):
    count = lax.axis_size(axes)
    return lax.all_to_all(
        jnp.broadcast_to(piece[None], (count, *piece.shape)), axes, 0, 0, tiled=True
    )


def from_tiles(tiles, rows, cols):
    return tiles.reshape(rows // 8, cols // 128, 8, 128).transpose(0, 2, 1, 3).reshape(rows, cols)


def pull(jacobian, weighted):
    return lax.dot_general(
        jacobian, weighted, (((0,), (0,)), ((), ())), preferred_element_type=jnp.float32
    )


def body(jacobian, probes, prior_std, obs_weight):
    flux_local = probes.shape[1]
    obs_local = jacobian.shape[0]
    columns = probes.shape[0] * probes.shape[2]
    half, far = flux_local // 2, lax.axis_index("zh").astype(jnp.uint32)
    rows = (far * obs_local, (1 - far) * obs_local, far * half)
    portion = flux_local // lax.axis_size(OBS_AXES)
    local_std = lax.dynamic_slice_in_dim(prior_std, lax.axis_index(OBS_AXES) * portion, portion)
    sent = lax.dynamic_slice_in_dim(jacobian, (1 - far) * half, half, 1)
    far_part = lax.ppermute(sent, "zh", ((0, 1), (1, 0)))
    tiles = forward_tiles(jacobian, probes, prior_std, obs_weight)
    moved = lax.all_to_all(tiles, FLUX_AXES, 0, 0, tiled=True)
    tile = jnp.sum(moved, axis=0)
    tile, local_std, rows = lax.optimization_barrier((tile, local_std, rows))
    near_part = lax.dynamic_slice_in_dim(jacobian, rows[2], half, 1)
    weighted = gather(tile.astype(jnp.bfloat16), ("zh",) + FLUX_AXES)
    weighted = from_tiles(weighted, 2 * obs_local, columns)
    adjoint = pull(near_part, lax.dynamic_slice_in_dim(weighted, rows[0], obs_local))
    adjoint += pull(far_part, lax.dynamic_slice_in_dim(weighted, rows[1], obs_local))
    adjoint = scatter_sum(adjoint.astype(jnp.bfloat16).reshape(-1, portion, columns), NEAR_OBS)
    sketch = adjoint * local_std[:, None]
    left, right = sketch[:, :HALF], sketch[:, HALF:]
    gram = jnp.concatenate(
        [dot(left, sketch, ((0,), (0,))), dot(right, right, ((0,), (0,)))], axis=1
    )
    slab = gram.astype(jnp.bfloat16).reshape(lax.axis_size(PLANE), -1, gram.shape[1])
    slab = lax.optimization_barrier(scatter_sum(slab, PLANE)).astype(jnp.bfloat16)
    slab = jnp.sum(gather(slab, LINE).astype(jnp.float32), axis=0)
    gram = gather(slab, PLANE)
    scale_root = math.sqrt(flux_local * lax.axis_size(FLUX_AXES))
    return (sketch, basis(gram, sketch, scale_root))


def solution(mesh):
    split = Mesh(mesh.devices.reshape(2, 4, 2, 8, 4), ("zh", "y", "c", "zl", "x"))
    in_specs = (P(OBS_AXES, FLUX_AXES), P(None, FLUX_AXES, None), P(FLUX_AXES), P(OBS_AXES))
    out_specs = (P(FLUX_AXES + OBS_AXES, None), P(FLUX_AXES + OBS_AXES, None))

    return jax.shard_map(body, mesh=split, in_specs=in_specs, out_specs=out_specs, check_vma=False)
```

```python
import functools
import math

import jax
import jax.numpy as jnp
from jax import lax
from jax.experimental import pallas as pl
from jax.experimental.pallas import tpu as pltpu
from jax.sharding import Mesh, PartitionSpec as P

OBS_AXES = ("zh", "y", "c")
FLUX_AXES = ("zl", "x")
NEAR_OBS = ("y", "c")
PLANE = ("y", "c", "x")
LINE = ("zh", "zl")
HALF = 128
STEP = 8
VMEM_LIMIT = 16 * 2**20
HIGHEST = lax.Precision.HIGHEST


def pick(values, index):
    return jnp.take_along_axis(values, index, axis=1, mode="promise_in_bounds")


def eliminate(diag, inverse, lanes, near):
    sub = lax.broadcasted_iota(jnp.int32, (STEP, HALF), 0)
    blocks = HALF // STEP
    columns = [pick(diag[:STEP, :], jnp.full((STEP, HALF), k, jnp.int32)) for k in range(STEP)]
    for t in range(blocks):
        top, low = t * STEP, (t + 1) * STEP
        base = t % 2 * STEP * STEP
        for k in range(STEP):
            lanes[base + k * STEP : base + (k + 1) * STEP, :] = columns[k]
        entry = {}
        for k in range(STEP):
            for j in range(k, STEP):
                entry[j, k] = lanes[pl.ds(base + k * STEP + j, STEP, stride=0), :]
        rows = [[ref[pl.ds(top + k, STEP, stride=0), :] for ref in (diag, inverse)] for k in range(STEP)]
        last = t + 1 == blocks
        if not last:
            below = diag[low : low + STEP, :]
            columns = [pick(below, jnp.full((STEP, HALF), low + k, jnp.int32)) for k in range(STEP)]
        for k in range(STEP):
            scale = lax.rsqrt(entry[k, k])
            rows[k] = [row * scale for row in rows[k]]
            mult = {j: entry[j, k] * scale for j in range(k + 1, STEP)}
            for j in range(k + 1, STEP):
                for i in range(j, STEP):
                    entry[i, j] = entry[i, j] - mult[i] * mult[j]
                rows[j] = [row - mult[j] * pivot for row, pivot in zip(rows[j], rows[k])]
            for ref, row in zip((inverse,), rows[k][1:]):
                ref[top + k : top + k + 1, :] = row[:1, :]
            if not last:
                mult = pick(rows[k][0], sub + low)
                spot = base + k * STEP
                near[spot : spot + STEP, :] = mult
                columns = [
                    column - mult * near[pl.ds(spot + j, STEP, stride=0), :]
                    for j, column in enumerate(columns)
                ]
        for block in range(t + 1, blocks):
            low = block * STEP
            index = sub + low
            work = [ref[low : low + STEP, :] for ref in (diag, inverse)]
            for k in range(STEP):
                if block == t + 1:
                    mult = near[base + k * STEP : base + (k + 1) * STEP, :]
                else:
                    mult = pick(rows[k][0], index)
                work = [row - mult * pivot for row, pivot in zip(work, rows[k])]
            for ref, row in zip((diag, inverse), work):
                ref[low : low + STEP, :] = row


def identity():
    shape = (HALF, HALF)
    return (lax.broadcasted_iota(jnp.int32, shape, 0) == lax.broadcasted_iota(jnp.int32, shape, 1)).astype(jnp.float32)


def dot(a, b, dims):
    return lax.dot_general(a, b, (dims, ((), ())), precision=HIGHEST, preferred_element_type=jnp.float32)


def basis_kernel(root, packed, sketch, out, gram, diag, low, high, lanes, near):
    rows = packed.shape[1]
    for k in range(packed.shape[0]):
        gram[k * rows : (k + 1) * rows, :] = packed[k]
    diag[...] = gram[:, :HALF]
    low[...] = identity()
    eliminate(diag, low, lanes, near)
    upper = dot(low[...], gram[:, HALF : 2 * HALF], ((1,), (0,)))
    diag[...] = gram[:, 2 * HALF :] - dot(upper, upper, ((0,), (0,)))
    high[...] = identity()
    eliminate(diag, high, lanes, near)
    first, second = sketch[:, :HALF], sketch[:, HALF:]
    left = dot(first, low[...], ((1,), (1,)))
    out[:, :HALF] = root * left
    rest = second - dot(left, upper, ((1,), (0,)))
    out[:, HALF:] = root * dot(rest, high[...], ((1,), (1,)))


def basis(gram, sketch, root):
    square = pltpu.VMEM((HALF, HALF), jnp.float32)
    vmem = pl.BlockSpec(memory_space=pltpu.VMEM)
    return pl.pallas_call(
        functools.partial(basis_kernel, root),
        out_shape=jax.ShapeDtypeStruct(sketch.shape, jnp.float32),
        in_specs=[vmem, vmem],
        out_specs=vmem,
        scratch_shapes=[pltpu.VMEM((HALF, 3 * HALF), jnp.float32), square, square, square, *[pltpu.VMEM((2 * STEP * STEP, HALF), jnp.float32)] * 2],
        compiler_params=pltpu.CompilerParams(vmem_limit_bytes=VMEM_LIMIT),
        name="cholesky_basis",
    )(gram, sketch)


def forward_kernel(
    far_jacobian, far_probes, far_spread, far_weight, far_out, jacobian, probes, spread, weight, out, sems
):
    sub = lax.broadcasted_iota(jnp.int32, (STEP, HALF), 0)
    blocks, flux_local, _ = probes.shape
    pair = 2 * STEP
    pairs = ((far_spread, spread), (far_probes, probes), (far_jacobian, jacobian), (far_weight, weight))
    copies = [pltpu.make_async_copy(*ends, sems.at[i]) for i, ends in enumerate(pairs)]
    for copy in copies:
        copy.start()
    for copy in copies:
        copy.wait()
    stacked = []
    for low in range(0, flux_local, pair):
        row = spread[pl.ds(low // HALF, STEP, stride=0), :]
        factor = jnp.concatenate([pick(row, sub + (low + half) % HALF) for half in (0, STEP)], axis=0)
        scaled = [probes[b, low : low + pair, :].astype(jnp.float32) * factor for b in range(blocks)]
        stacked.append(jnp.concatenate([block.astype(jnp.bfloat16) for block in scaled], axis=1))
    stacked = jnp.concatenate(stacked, axis=0)
    row = weight[pl.ds(0, STEP, stride=0), :]
    total = jnp.dot(jacobian[...], stacked, preferred_element_type=jnp.float32)
    for k in range(out.shape[0]):
        r, c = k // blocks * STEP, k % blocks * HALF
        out[k] = total[r : r + STEP, c : c + HALF] * pick(row, sub + r)
    result = pltpu.make_async_copy(out, far_out, sems.at[0])
    result.start()
    result.wait()


def forward_tiles(jacobian, probes, prior_std, obs_weight):
    rows, flux_local = jacobian.shape
    columns = probes.shape[0] * probes.shape[2]
    spread = prior_std.reshape(flux_local // HALF, HALF)
    hbm = pl.BlockSpec(memory_space=pltpu.MemorySpace.HBM)
    shape = (rows * columns // (STEP * HALF), STEP, HALF)
    return pl.pallas_call(
        forward_kernel,
        out_shape=jax.ShapeDtypeStruct(shape, jnp.float32),
        in_specs=[hbm] * 4,
        out_specs=hbm,
        scratch_shapes=[
            pltpu.VMEM(jacobian.shape, jacobian.dtype),
            pltpu.VMEM(probes.shape, probes.dtype),
            pltpu.VMEM(spread.shape, spread.dtype),
            pltpu.VMEM((1, rows), jnp.float32),
            pltpu.VMEM(shape, jnp.float32),
            pltpu.SemaphoreType.DMA((4,)),
        ],
        name="forward_tiles",
    )(jacobian, probes, spread, obs_weight.reshape(1, rows))


def scatter_sum(parts, axes):
    moved = lax.all_to_all(parts, axes, 0, 0, tiled=True)
    return jnp.sum(moved.astype(jnp.float32), axis=0)


def gather(piece, axes):
    count = lax.axis_size(axes)
    return lax.all_to_all(
        jnp.broadcast_to(piece[None], (count, *piece.shape)), axes, 0, 0, tiled=True
    )


def from_tiles(tiles, rows, cols):
    return tiles.reshape(rows // 8, cols // 128, 8, 128).transpose(0, 2, 1, 3).reshape(rows, cols)


def pull(jacobian, weighted):
    return lax.dot_general(
        jacobian, weighted, (((0,), (0,)), ((), ())), preferred_element_type=jnp.float32
    )


def body(jacobian, probes, prior_std, obs_weight):
    flux_local = probes.shape[1]
    obs_local = jacobian.shape[0]
    columns = probes.shape[0] * probes.shape[2]
    half, far = flux_local // 2, lax.axis_index("zh").astype(jnp.uint32)
    rows = (far * obs_local, (1 - far) * obs_local, far * half)
    portion = flux_local // lax.axis_size(OBS_AXES)
    local_std = lax.dynamic_slice_in_dim(prior_std, lax.axis_index(OBS_AXES) * portion, portion)
    sent = lax.dynamic_slice_in_dim(jacobian, (1 - far) * half, half, 1)
    far_part = lax.ppermute(sent, "zh", ((0, 1), (1, 0)))
    tiles = forward_tiles(jacobian, probes, prior_std, obs_weight)
    moved = lax.all_to_all(tiles, FLUX_AXES, 0, 0, tiled=True)
    tile = jnp.sum(moved, axis=0)
    tile, local_std, rows = lax.optimization_barrier((tile, local_std, rows))
    near_part = lax.dynamic_slice_in_dim(jacobian, rows[2], half, 1)
    weighted = gather(tile.astype(jnp.bfloat16), ("zh",) + FLUX_AXES)
    weighted = from_tiles(weighted, 2 * obs_local, columns)
    adjoint = pull(near_part, lax.dynamic_slice_in_dim(weighted, rows[0], obs_local))
    adjoint += pull(far_part, lax.dynamic_slice_in_dim(weighted, rows[1], obs_local))
    adjoint = scatter_sum(adjoint.astype(jnp.bfloat16).reshape(-1, portion, columns), NEAR_OBS)
    sketch = adjoint * local_std[:, None]
    gram = lax.dot_general(
        sketch, sketch, (((0,), (0,)), ((), ())),
        precision=lax.Precision.HIGH, preferred_element_type=jnp.float32,
    )
    gram = jnp.concatenate([gram[:HALF], gram[HALF:, HALF:]], axis=1)
    slab = gram.astype(jnp.bfloat16).reshape(lax.axis_size(PLANE), -1, gram.shape[1])
    slab = lax.optimization_barrier(scatter_sum(slab, PLANE)).astype(jnp.bfloat16)
    slab = jnp.sum(gather(slab, LINE).astype(jnp.float32), axis=0)
    gram = gather(slab, PLANE)
    scale_root = math.sqrt(flux_local * lax.axis_size(FLUX_AXES))
    return (sketch, basis(gram, sketch, scale_root))


def solution(mesh):
    split = Mesh(mesh.devices.reshape(2, 4, 2, 8, 4), ("zh", "y", "c", "zl", "x"))
    in_specs = (P(OBS_AXES, FLUX_AXES), P(None, FLUX_AXES, None), P(FLUX_AXES), P(OBS_AXES))
    out_specs = (P(FLUX_AXES + OBS_AXES, None), P(FLUX_AXES + OBS_AXES, None))

    return jax.shard_map(body, mesh=split, in_specs=in_specs, out_specs=out_specs, check_vma=False)
```

```python
import functools
import math

import jax
import jax.numpy as jnp
from jax import lax
from jax.experimental import pallas as pl
from jax.experimental.pallas import tpu as pltpu
from jax.sharding import Mesh, PartitionSpec as P

OBS_AXES = ("zh", "y", "c")
FLUX_AXES = ("zl", "x")
NEAR_OBS = ("y", "c")
PLANE = ("y", "c", "x")
LINE = ("zh", "zl")
HALF = 128
STEP = 8
VMEM_LIMIT = 16 * 2**20
HIGHEST = lax.Precision.HIGHEST


def pick(values, index):
    return jnp.take_along_axis(values, index, axis=1, mode="promise_in_bounds")


def eliminate(diag, inverse, lanes, near):
    sub = lax.broadcasted_iota(jnp.int32, (STEP, HALF), 0)
    blocks = HALF // STEP
    columns = [pick(diag[:STEP, :], jnp.full((STEP, HALF), k, jnp.int32)) for k in range(STEP)]
    for t in range(blocks):
        top, low = t * STEP, (t + 1) * STEP
        base = t % 2 * STEP * STEP
        for k in range(STEP):
            lanes[base + k * STEP : base + (k + 1) * STEP, :] = columns[k]
        entry = {}
        for k in range(STEP):
            for j in range(k, STEP):
                entry[j, k] = lanes[pl.ds(base + k * STEP + j, STEP, stride=0), :]
        rows = [[ref[pl.ds(top + k, STEP, stride=0), :] for ref in (diag, inverse)] for k in range(STEP)]
        last = t + 1 == blocks
        if not last:
            below = diag[low : low + STEP, :]
            columns = [pick(below, jnp.full((STEP, HALF), low + k, jnp.int32)) for k in range(STEP)]
        for k in range(STEP):
            scale = lax.rsqrt(entry[k, k])
            rows[k] = [row * scale for row in rows[k]]
            mult = {j: entry[j, k] * scale for j in range(k + 1, STEP)}
            for j in range(k + 1, STEP):
                for i in range(j, STEP):
                    entry[i, j] = entry[i, j] - mult[i] * mult[j]
                rows[j] = [row - mult[j] * pivot for row, pivot in zip(rows[j], rows[k])]
            for ref, row in zip((inverse,), rows[k][1:]):
                ref[top + k : top + k + 1, :] = row[:1, :]
            if not last:
                mult = pick(rows[k][0], sub + low)
                spot = base + k * STEP
                near[spot : spot + STEP, :] = mult
                columns = [
                    column - mult * near[pl.ds(spot + j, STEP, stride=0), :]
                    for j, column in enumerate(columns)
                ]
        for block in range(t + 1, blocks):
            low = block * STEP
            index = sub + low
            work = [ref[low : low + STEP, :] for ref in (diag, inverse)]
            for k in range(STEP):
                if block == t + 1:
                    mult = near[base + k * STEP : base + (k + 1) * STEP, :]
                else:
                    mult = pick(rows[k][0], index)
                work = [row - mult * pivot for row, pivot in zip(work, rows[k])]
            for ref, row in zip((diag, inverse), work):
                ref[low : low + STEP, :] = row


def identity():
    shape = (HALF, HALF)
    return (lax.broadcasted_iota(jnp.int32, shape, 0) == lax.broadcasted_iota(jnp.int32, shape, 1)).astype(jnp.float32)


def dot(a, b, dims):
    return lax.dot_general(a, b, (dims, ((), ())), precision=HIGHEST, preferred_element_type=jnp.float32)


def basis_kernel(root, packed, sketch, out, gram, diag, low, high, lanes, near):
    rows = packed.shape[1]
    for k in range(packed.shape[0]):
        gram[k * rows : (k + 1) * rows, :] = packed[k]
    diag[...] = gram[:, :HALF]
    low[...] = identity()
    eliminate(diag, low, lanes, near)
    upper = dot(low[...], gram[:, HALF : 2 * HALF], ((1,), (0,)))
    diag[...] = gram[:, 2 * HALF :] - dot(upper, upper, ((0,), (0,)))
    high[...] = identity()
    eliminate(diag, high, lanes, near)
    first, second = sketch[:, :HALF], sketch[:, HALF:]
    left = dot(first, low[...], ((1,), (1,)))
    out[:, :HALF] = root * left
    rest = second - dot(left, upper, ((1,), (0,)))
    out[:, HALF:] = root * dot(rest, high[...], ((1,), (1,)))


def basis(gram, sketch, root):
    square = pltpu.VMEM((HALF, HALF), jnp.float32)
    vmem = pl.BlockSpec(memory_space=pltpu.VMEM)
    return pl.pallas_call(
        functools.partial(basis_kernel, root),
        out_shape=jax.ShapeDtypeStruct(sketch.shape, jnp.float32),
        in_specs=[vmem, vmem],
        out_specs=vmem,
        scratch_shapes=[pltpu.VMEM((HALF, 3 * HALF), jnp.float32), square, square, square, *[pltpu.VMEM((2 * STEP * STEP, HALF), jnp.float32)] * 2],
        compiler_params=pltpu.CompilerParams(vmem_limit_bytes=VMEM_LIMIT),
        name="cholesky_basis",
    )(gram, sketch)


def forward_kernel(
    far_jacobian, far_probes, far_spread, far_weight, far_out, jacobian, probes, spread, weight, out, sems
):
    sub = lax.broadcasted_iota(jnp.int32, (STEP, HALF), 0)
    blocks, flux_local, _ = probes.shape
    pair = 2 * STEP
    pairs = ((far_spread, spread), (far_probes, probes), (far_jacobian, jacobian), (far_weight, weight))
    copies = [pltpu.make_async_copy(*ends, sems.at[i]) for i, ends in enumerate(pairs)]
    for copy in copies:
        copy.start()
    for copy in copies:
        copy.wait()
    stacked = []
    for low in range(0, flux_local, pair):
        row = spread[pl.ds(low // HALF, STEP, stride=0), :]
        factor = jnp.concatenate([pick(row, sub + (low + half) % HALF) for half in (0, STEP)], axis=0)
        scaled = [probes[b, low : low + pair, :].astype(jnp.float32) * factor for b in range(blocks)]
        stacked.append(jnp.concatenate([block.astype(jnp.bfloat16) for block in scaled], axis=1))
    stacked = jnp.concatenate(stacked, axis=0)
    row = weight[pl.ds(0, STEP, stride=0), :]
    total = jnp.dot(jacobian[...], stacked, preferred_element_type=jnp.float32)
    for k in range(out.shape[0]):
        r, c = k // blocks * STEP, k % blocks * HALF
        out[k] = total[r : r + STEP, c : c + HALF] * pick(row, sub + r)
    result = pltpu.make_async_copy(out, far_out, sems.at[0])
    result.start()
    result.wait()


def forward_tiles(jacobian, probes, prior_std, obs_weight):
    rows, flux_local = jacobian.shape
    columns = probes.shape[0] * probes.shape[2]
    spread = prior_std.reshape(flux_local // HALF, HALF)
    hbm = pl.BlockSpec(memory_space=pltpu.MemorySpace.HBM)
    shape = (rows * columns // (STEP * HALF), STEP, HALF)
    return pl.pallas_call(
        forward_kernel,
        out_shape=jax.ShapeDtypeStruct(shape, jnp.float32),
        in_specs=[hbm] * 4,
        out_specs=hbm,
        scratch_shapes=[
            pltpu.VMEM(jacobian.shape, jacobian.dtype),
            pltpu.VMEM(probes.shape, probes.dtype),
            pltpu.VMEM(spread.shape, spread.dtype),
            pltpu.VMEM((1, rows), jnp.float32),
            pltpu.VMEM(shape, jnp.float32),
            pltpu.SemaphoreType.DMA((4,)),
        ],
        name="forward_tiles",
    )(jacobian, probes, spread, obs_weight.reshape(1, rows))


def scatter_sum(parts, axes):
    moved = lax.all_to_all(parts, axes, 0, 0, tiled=True)
    return jnp.sum(moved.astype(jnp.float32), axis=0)


def gather(piece, axes):
    count = lax.axis_size(axes)
    return lax.all_to_all(
        jnp.broadcast_to(piece[None], (count, *piece.shape)), axes, 0, 0, tiled=True
    )


def from_tiles(tiles, rows, cols):
    return tiles.reshape(rows // 8, cols // 128, 8, 128).transpose(0, 2, 1, 3).reshape(rows, cols)


def pull(jacobian, weighted):
    return lax.dot_general(
        jacobian, weighted, (((0,), (0,)), ((), ())), preferred_element_type=jnp.float32
    )


def body(jacobian, probes, prior_std, obs_weight):
    flux_local = probes.shape[1]
    obs_local = jacobian.shape[0]
    columns = probes.shape[0] * probes.shape[2]
    half, far = flux_local // 2, lax.axis_index("zh").astype(jnp.uint32)
    rows = (far * obs_local, (1 - far) * obs_local, far * half)
    portion = flux_local // lax.axis_size(OBS_AXES)
    local_std = lax.dynamic_slice_in_dim(prior_std, lax.axis_index(OBS_AXES) * portion, portion)
    sent = lax.dynamic_slice_in_dim(jacobian, (1 - far) * half, half, 1)
    far_part = lax.ppermute(sent, "zh", ((0, 1), (1, 0)))
    tiles = forward_tiles(jacobian, probes, prior_std, obs_weight)
    moved = lax.all_to_all(tiles, FLUX_AXES, 0, 0, tiled=True)
    tile = jnp.sum(moved, axis=0)
    near_part = lax.dynamic_slice_in_dim(jacobian, rows[2], half, 1)
    tile, local_std, rows, near_part = lax.optimization_barrier((tile, local_std, rows, near_part))
    weighted = gather(tile.astype(jnp.bfloat16), ("zh",) + FLUX_AXES)
    weighted = from_tiles(weighted, 2 * obs_local, columns)
    parts = [lax.dynamic_slice_in_dim(weighted, row, obs_local) for row in rows[:2]]
    adjoint = pull(jnp.concatenate([near_part, far_part]), jnp.concatenate(parts))
    adjoint = scatter_sum(adjoint.astype(jnp.bfloat16).reshape(-1, portion, columns), NEAR_OBS)
    sketch = adjoint * local_std[:, None]
    gram = lax.dot_general(
        sketch, sketch, (((0,), (0,)), ((), ())),
        precision=lax.Precision.HIGH, preferred_element_type=jnp.float32,
    )
    gram = jnp.concatenate([gram[:HALF], gram[HALF:, HALF:]], axis=1)
    slab = gram.astype(jnp.bfloat16).reshape(lax.axis_size(PLANE), -1, gram.shape[1])
    slab = lax.optimization_barrier(scatter_sum(slab, PLANE)).astype(jnp.bfloat16)
    slab = jnp.sum(gather(slab, LINE).astype(jnp.float32), axis=0)
    gram = gather(slab, PLANE)
    scale_root = math.sqrt(flux_local * lax.axis_size(FLUX_AXES))
    return (sketch, basis(gram, sketch, scale_root))


def solution(mesh):
    split = Mesh(mesh.devices.reshape(2, 4, 2, 8, 4), ("zh", "y", "c", "zl", "x"))
    in_specs = (P(OBS_AXES, FLUX_AXES), P(None, FLUX_AXES, None), P(FLUX_AXES), P(OBS_AXES))
    out_specs = (P(FLUX_AXES + OBS_AXES, None), P(FLUX_AXES + OBS_AXES, None))

    return jax.shard_map(body, mesh=split, in_specs=in_specs, out_specs=out_specs, check_vma=False)
```
